32 devices in a mesh: ifg: 16 (over z, y, x), slab: 2 (over core).
Axes of the slice: x: 2, y: 2, z: 4, core: 2. Of those that a mesh axis runs over, the one named last changes fastest.
Arguments:
- phase: float32 [2, 1152, 6144], P('slab', 'ifg'), may hold values from -60 to 60
- corrections: int32 [2, 1152, 6144], P('slab', 'ifg'), may hold values from -1 to 1
- closure_loops: int32 [288, 1152], replicated, may hold values from -1 to 1, as said below
- design: int32 [1152, 288], replicated, may hold values from -1 to 1, as said below
Outputs:
- closure_phase: float32 [2, 288, 6144], P('slab', None, 'ifg')
- displacement: float32 [2, 288, 6144], P('slab', None, 'ifg')
- misfit: float32 [2], P('slab')
The draws below stay inside these ranges and needn't reach their ends.
Inputs may be any that keep to these rules, and one draw needn't show every extreme that they name: Each row of closure_loops holds +1 at two interferograms and -1 at a third; closure_loops times design is zero. Each row of design holds one +1 and one -1 in different columns; every date is named by some row.
All inputs are finite; a program needn't handle non-finite values.
Results may differ from the reference program's by a relative error of at most 0.0003.
Values sent between devices are 32-bit elements; how exact they have to be, the bound alone decides.
A program may use at most 64 MiB of HBM per device.

```python
import jax
import jax.numpy as jnp
from jax import lax

DATES = 288
IFGS = 1152
SLAB_PIX = 6144
SLABS = 2


two_pi = 6.283185307179586


def network(key):
    anchor = jnp.arange(DATES, dtype=jnp.int32)
    offsets = jax.random.randint(jax.random.fold_in(key, 11), (3, DATES), 1, 5)
    middle = (anchor + offsets[0]) % DATES
    finish = (anchor + offsets[0] + offsets[1]) % DATES
    spur_end = (anchor + offsets[2] + 4) % DATES
    start_dates = jnp.concatenate([anchor, middle, anchor, anchor])
    end_dates = jnp.concatenate([middle, finish, finish, spur_end])
    reorder = jax.random.permutation(jax.random.fold_in(key, 12), IFGS).astype(jnp.int32)
    columns = jnp.arange(DATES, dtype=jnp.int32)[None, :]
    design = (columns == end_dates[reorder][:, None]).astype(jnp.int32) - (columns == start_dates[reorder][:, None]).astype(jnp.int32)
    loop_ids = jnp.arange(DATES, dtype=jnp.int32)[:, None]
    source = reorder[None, :]
    closure = (source == loop_ids).astype(jnp.int32) + (source == loop_ids + DATES).astype(jnp.int32) - (source == loop_ids + 2 * DATES).astype(jnp.int32)
    return (closure, design)


def jump_counts(key):
    level = jax.random.randint(jax.random.fold_in(key, 21), (SLABS, IFGS, SLAB_PIX), 0, 10)
    return jnp.where(level == 0, -1, jnp.where(level == 9, 1, 0)).astype(jnp.int32)


def draw_closure_loops(key, part):
    return network(jax.random.fold_in(key, 5))[0]


def draw_design(key, part):
    return network(jax.random.fold_in(key, 5))[1]


def draw_corrections(key, part):
    return jump_counts(jax.random.fold_in(key, 6))


def draw_phase(key, part):
    closure, design = network(jax.random.fold_in(key, 5))
    design_float = design.astype(jnp.float32)
    counts = jump_counts(jax.random.fold_in(key, 6)).astype(jnp.float32)
    rising = 1.0 + 2.0 * jnp.arange(SLAB_PIX, dtype=jnp.float32) / SLAB_PIX
    epochs = jnp.arange(1, DATES + 1, dtype=jnp.float32) / DATES
    base = jax.random.fold_in(key, 31)
    slab_offset = 0.6 * jnp.arange(SLABS, dtype=jnp.float32) + 0.4 * jax.random.uniform(jax.random.fold_in(base, 4), (SLABS,), jnp.float32, 0.0, 1.0)
    rate = 0.5 * jnp.clip(jax.random.normal(jax.random.fold_in(base, 1), (SLABS, SLAB_PIX), jnp.float32), -4.0, 4.0) + 1.5 * rising[None, :] + slab_offset[:, None]
    weather = 0.5 * jnp.clip(jax.random.normal(jax.random.fold_in(base, 2), (SLABS, DATES, SLAB_PIX), jnp.float32), -4.0, 4.0)
    noise_part = 0.2 * rising[None, None, :] * jnp.clip(jax.random.normal(jax.random.fold_in(base, 3), (SLABS, IFGS, SLAB_PIX), jnp.float32), -4.0, 4.0)
    truth = 3.0 * rate[:, None, :] * epochs[None, :, None] + weather
    signal = jnp.einsum('md,sdp->smp', design_float, truth)
    return signal + noise_part - two_pi * counts


def setup_inputs(seed: int = 0) -> dict:
    arg_keys = jax.random.split(jax.random.key(seed), 5)
    phase = draw_phase(jax.random.fold_in(arg_keys[4], 71), 0)
    corrections = draw_corrections(jax.random.fold_in(arg_keys[4], 71), 0)
    closure_loops = draw_closure_loops(jax.random.fold_in(arg_keys[4], 71), 0)
    design = draw_design(jax.random.fold_in(arg_keys[4], 71), 0)
    return {"phase": phase, "corrections": corrections, "closure_loops": closure_loops, "design": design}


ridge_weight = 1.0
two_pi = 6.283185307179586
epsilon = 1e-06
highest = lax.Precision.HIGHEST

def reference(phase, corrections, closure_loops, design):
    loop_rows = closure_loops.astype(jnp.float32)
    design_float = design.astype(jnp.float32)
    normal = jnp.dot(design_float.T, design_float, precision=highest) + ridge_weight * jnp.eye(DATES, dtype=jnp.float32)

    def one_slab(members):
        phase_rows, counts = members
        corrected = phase_rows + two_pi * counts.astype(jnp.float32)
        closure = jnp.dot(loop_rows, corrected, precision=highest)
        projected = jnp.dot(design_float.T, corrected, precision=highest)
        shifts = jnp.linalg.solve(normal, projected)
        residual = corrected - jnp.dot(design_float, shifts, precision=highest)
        return (closure, shifts, jnp.sum(residual * residual))
    closure_phase, shifts, slab_square = lax.map(one_slab, (phase, corrections))
    frame_mean = lax.optimization_barrier(jnp.sum(shifts, axis=(0, 2))) / (SLABS * SLAB_PIX)
    displacement = shifts - frame_mean[None, :, None]
    misfit = jnp.sqrt(slab_square / (IFGS * SLAB_PIX) + epsilon)
    return (closure_phase, displacement, misfit)
```

```python
import functools

import jax
import jax.numpy as jnp
from jax import lax
from jax.experimental import pallas as pl
from jax.experimental.pallas import tpu as pltpu
from jax.sharding import PartitionSpec as P

ridge_weight = 1.0
two_pi = 6.283185307179586
epsilon = 1e-06
highest = lax.Precision.HIGHEST
f32 = jnp.float32
bf16 = jnp.bfloat16
MESH = pl.DeviceIdType.MESH
newton_steps = 2


def dot(a, b):
    return jnp.dot(a, b, preferred_element_type=f32)


def split(a):
    high = a.astype(bf16)
    return high, (a - high.astype(f32)).astype(bf16)


def split_three(a):
    high = a.astype(bf16)
    rest = a - high.astype(f32)
    middle = rest.astype(bf16)
    return high, middle, (rest - middle.astype(f32)).astype(bf16)


def dot_split(a, b):
    a_high, a_low = split(a)
    b_high, b_low = split(b)
    return dot(a_high, b_high) + (dot(a_high, b_low) + dot(a_low, b_high))


def partner(me, k, n):
    if n & (n - 1):
        return lax.rem(me + k, n)
    out, bit = 0, 1
    while bit < n:
        out = out + bit * (((me // bit) % 2 + (k // bit) % 2) % 2)
        bit *= 2
    return out


def kernel(n, slabs, widths, doublings, phase, counts, loops, design, closure_out, shifts_out, total_out,
           phase_v, counts_v, sent, *rest):
    chunk_count = len(widths)
    got, rest = rest[:chunk_count], rest[chunk_count:]
    (loops_v, design_v, design_b, left, stack, normal, row, rows_in, flat,
     in_sem, table_sem, own_sem, send_sem, recv_sem, row_send, row_recv) = rest
    me = lax.axis_index("ifg")
    slab = lax.axis_index("slab")
    rows = phase.shape[1]
    dates = design.shape[1]
    columns = sum(widths)
    starts = [sum(widths[:c]) for c in range(chunk_count)]

    loads = [
        pltpu.make_async_copy(phase.at[0], phase_v, in_sem.at[0]),
        pltpu.make_async_copy(counts.at[0], counts_v, in_sem.at[1]),
    ]
    tables = [
        pltpu.make_async_copy(design, design_v, table_sem.at[0]),
        pltpu.make_async_copy(loops, loops_v, table_sem.at[1]),
    ]
    for copy in loads:
        copy.start()

    barrier = pltpu.get_barrier_semaphore()
    for other in range(slabs):
        far_slab = lax.rem(slab + other, slabs)

        @pl.loop(0 if other else 1, n)
        def _(k):
            pl.semaphore_signal(
                barrier, inc=1, device_id={"ifg": partner(me, k, n), "slab": far_slab}, device_id_type=MESH
            )

    for copy in tables:
        copy.start()
    for copy in loads:
        copy.wait()
    sent[...] = phase_v[...] + two_pi * counts_v[...].astype(f32)
    pl.semaphore_wait(barrier, n * slabs - 1)

    for c in range(chunk_count):
        @pl.loop(0, n - 1)
        def _(step):
            to = partner(me, n - 1 - step, n)
            pltpu.make_async_remote_copy(
                src_ref=sent.at[:, pl.ds(pl.multiple_of(to * columns + starts[c], 128), widths[c])],
                dst_ref=got[c].at[me],
                send_sem=send_sem.at[c],
                recv_sem=recv_sem.at[c],
                device_id={"ifg": to},
                device_id_type=MESH,
            ).start()

    own = [
        pltpu.make_async_copy(
            sent.at[:, pl.ds(pl.multiple_of(me * columns + starts[c], 128), widths[c])], got[c].at[me], own_sem.at[c]
        )
        for c in range(chunk_count)
    ]
    for copy in own:
        copy.start()

    eye_bool = lax.broadcasted_iota(jnp.int32, (dates, dates), 0) == lax.broadcasted_iota(
        jnp.int32, (dates, dates), 1
    )
    eye = eye_bool.astype(f32)
    for copy in tables:
        copy.wait()
    loop_count = loops.shape[0]
    left[0:loop_count, :] = loops_v[...].astype(f32).astype(bf16)
    design_b[...] = design_v[...].astype(f32).astype(bf16)
    left[loop_count:, :] = lax.dot_general(
        eye.astype(bf16), design_b[...], (((1,), (1,)), ((), ())), preferred_element_type=f32
    ).astype(bf16)
    matrix = dot(left[loop_count:, :], design_b[...]) + ridge_weight * eye
    normal[...] = matrix
    bound = jnp.max(jnp.sum(jnp.abs(matrix), axis=1, keepdims=True), axis=0, keepdims=True)
    scale = 2.0 / (bound + ridge_weight)
    stack[0:dates, :] = scale * eye
    stack[dates:, :] = eye - scale * matrix

    @pl.loop(0, doublings)
    def _(step):
        both = stack[...]
        product = dot_split(both, both[dates:, :])
        stack[0:dates, :] = both[0:dates, :] + product[0:dates, :]
        stack[dates:, :] = product[dates:, :]

    @pl.loop(0, newton_steps)
    def _(step):
        inverse = stack[0:dates, :]
        error = eye - jnp.dot(normal[...], inverse, precision=highest)
        stack[0:dates, :] = inverse + jnp.dot(inverse, error, precision=highest)

    squares = jnp.zeros((1, 128), f32)
    date_sums = jnp.zeros((8, dates), f32)
    for c in range(chunk_count):
        width = widths[c]
        own[c].wait()
        pltpu.make_async_copy(got[c].at[pl.ds(0, n - 1)], got[c].at[pl.ds(0, n - 1)], recv_sem.at[c]).wait()
        if rows % 8 == 0:
            held = got[c][...].reshape(n * rows, width)
        else:
            for source in range(n):
                flat[source * rows:(source + 1) * rows, 0:width] = got[c][source]
            held = flat[:, 0:width]
        triple = dot(left[...], jnp.concatenate(split_three(held), axis=1))
        summed = triple[:, 0:width] + (triple[:, width:2 * width] + triple[:, 2 * width:])
        closure_out[:, starts[c]:starts[c] + width] = summed[0:loop_count, :]
        shifts = jnp.dot(stack[0:dates, :], summed[loop_count:, :], precision=highest)
        shifts_out[:, starts[c]:starts[c] + width] = shifts
        modelled = dot(design_b[...], jnp.concatenate(split_three(shifts), axis=1))
        residual = held - (modelled[:, 0:width] + (modelled[:, width:2 * width] + modelled[:, 2 * width:]))
        line = jnp.sum(residual * residual, axis=0, keepdims=True)
        for part in range(width // 128):
            squares = squares + line[:, part * 128:(part + 1) * 128]
        date_sums = date_sums + lax.dot_general(
            jnp.ones((8, width), f32), shifts, (((1,), (1,)), ((), ())), precision=highest,
            preferred_element_type=f32,
        )

    padded = row.shape[2] - 128
    row[0, :, 0:dates] = date_sums[0:1, :]
    row[0, :, padded:] = squares
    mine = slab * n + me
    rows_in[mine, :, :] = row[0]
    for other in range(slabs):
        far_slab = lax.rem(slab + other, slabs)

        @pl.loop(0 if other else 1, n)
        def _(k):
            pltpu.make_async_remote_copy(
                src_ref=row.at[0],
                dst_ref=rows_in.at[mine],
                send_sem=row_send,
                recv_sem=row_recv,
                device_id={"ifg": partner(me, k, n), "slab": far_slab},
                device_id_type=MESH,
            ).start()

    for c in range(chunk_count):
        pltpu.make_async_copy(got[c].at[pl.ds(0, n - 1)], got[c].at[pl.ds(0, n - 1)], send_sem.at[c]).wait()
    everyone = rows_in.at[pl.ds(0, n * slabs - 1)]
    pltpu.make_async_copy(everyone, everyone, row_recv).wait()
    pltpu.make_async_copy(everyone, everyone, row_send).wait()
    total_out[:, 0:padded] = jnp.sum(rows_in[:, :, 0:padded], axis=0)
    total_out[:, padded:] = jnp.sum(rows_in[pl.ds(slab * n, n), :, padded:], axis=0)


def local(phase, corrections, closure_loops, design):
    n = lax.axis_size("ifg")
    slabs = lax.axis_size("slab")
    rows, pixels = phase.shape[1:]
    ifgs, dates = design.shape
    loop_count = closure_loops.shape[0]
    columns = pixels // n
    widths = (columns - 128, 128) if columns > 128 else (columns,)
    padded = -(-dates // 128) * 128
    doublings = 1
    while 2 ** doublings < 4 * ifgs:
        doublings += 1
    vmem = pl.BlockSpec(memory_space=pltpu.VMEM)
    anywhere = pl.BlockSpec(memory_space=pl.ANY)
    dma = pltpu.SemaphoreType.DMA
    closure, shifts, total = pl.pallas_call(
        functools.partial(kernel, n, slabs, widths, doublings),
        out_shape=(
            jax.ShapeDtypeStruct((loop_count, columns), f32),
            jax.ShapeDtypeStruct((dates, columns), f32),
            jax.ShapeDtypeStruct((1, padded + 128), f32),
        ),
        in_specs=[anywhere] * 4,
        out_specs=(vmem, vmem, vmem),
        scratch_shapes=[
            pltpu.VMEM((rows, pixels), f32),
            pltpu.VMEM((rows, pixels), jnp.int32),
            pltpu.VMEM((rows, pixels), f32),
            *[pltpu.VMEM((n, rows, width), f32) for width in widths],
            pltpu.VMEM((loop_count, ifgs), jnp.int32),
            pltpu.VMEM((ifgs, dates), jnp.int32),
            pltpu.VMEM((ifgs, dates), bf16),
            pltpu.VMEM((loop_count + dates, ifgs), bf16),
            pltpu.VMEM((2 * dates, dates), f32),
            pltpu.VMEM((dates, dates), f32),
            pltpu.VMEM((1, 1, padded + 128), f32),
            pltpu.VMEM((n * slabs, 1, padded + 128), f32),
            pltpu.VMEM((8 if rows % 8 == 0 else ifgs, max(widths)), f32),
            dma((2,)),
            dma((2,)),
            dma((len(widths),)),
            dma((len(widths),)),
            dma((len(widths),)),
            dma,
            dma,
        ],
        compiler_params=pltpu.CompilerParams(
            collective_id=0, has_side_effects=True, vmem_limit_bytes=48 * 1024 * 1024
        ),
    )(phase, corrections, closure_loops, design)
    frame_mean = total[0, 0:dates] / (slabs * pixels)
    displacement = shifts - frame_mean[:, None]
    misfit = jnp.sqrt(jnp.sum(total[0, padded:]) / (ifgs * pixels) + epsilon)
    return (closure[None], displacement[None], misfit.reshape(1))


def solution(mesh):
    in_specs = (P("slab", "ifg", None), P("slab", "ifg", None), P(), P())
    out_specs = (P("slab", None, "ifg"), P("slab", None, "ifg"), P("slab"))
    return jax.shard_map(local, mesh=mesh, in_specs=in_specs, out_specs=out_specs, check_vma=False)
```

```python
import functools

import jax
import jax.numpy as jnp
from jax import lax
from jax.experimental import pallas as pl
from jax.experimental.pallas import tpu as pltpu
from jax.sharding import PartitionSpec as P

ridge_weight = 1.0
two_pi = 6.283185307179586
epsilon = 1e-06
highest = lax.Precision.HIGHEST
f32 = jnp.float32
bf16 = jnp.bfloat16
MESH = pl.DeviceIdType.MESH
newton_steps = 2


def dot(a, b):
    return jnp.dot(a, b, preferred_element_type=f32)


def split(a):
    high = a.astype(bf16)
    return high, (a - high.astype(f32)).astype(bf16)


def split_three(a):
    high = a.astype(bf16)
    rest = a - high.astype(f32)
    middle = rest.astype(bf16)
    return high, middle, (rest - middle.astype(f32)).astype(bf16)


def dot_split(a, b):
    a_high, a_low = split(a)
    b_high, b_low = split(b)
    return dot(a_high, b_high) + (dot(a_high, b_low) + dot(a_low, b_high))


def partner(me, k, n):
    if n & (n - 1):
        return lax.rem(me + k, n)
    out, bit = 0, 1
    while bit < n:
        out = out + bit * (((me // bit) % 2 + (k // bit) % 2) % 2)
        bit *= 2
    return out


def kernel(n, slabs, widths, doublings, phase, counts, loops, design_t, closure_out, shifts_out, misfit_out,
           phase_v, counts_v, sent, *rest):
    chunk_count = len(widths)
    got, rest = rest[:chunk_count], rest[chunk_count:]
    (loops_v, design_v, design_b, left, stack, normal, row, rows_in, flat,
     in_sem, table_sem, own_sem, send_sem, recv_sem, row_send, row_recv) = rest
    me = lax.axis_index("ifg")
    slab = lax.axis_index("slab")
    rows = phase.shape[1]
    dates, ifgs = design_t.shape
    columns = sum(widths)
    starts = [sum(widths[:c]) for c in range(chunk_count)]

    loads = [
        pltpu.make_async_copy(phase.at[0], phase_v, in_sem.at[0]),
        pltpu.make_async_copy(counts.at[0], counts_v, in_sem.at[1]),
    ]
    tables = [
        pltpu.make_async_copy(design_t, design_v, table_sem.at[0]),
        pltpu.make_async_copy(loops, loops_v, table_sem.at[1]),
    ]
    for copy in loads:
        copy.start()

    barrier = pltpu.get_barrier_semaphore()
    for other in range(slabs):
        far_slab = lax.rem(slab + other, slabs)

        @pl.loop(0 if other else 1, n)
        def _(k):
            pl.semaphore_signal(
                barrier, inc=1, device_id={"ifg": partner(me, k, n), "slab": far_slab}, device_id_type=MESH
            )

    for copy in tables:
        copy.start()
    for copy in loads:
        copy.wait()
    sent[...] = phase_v[...] + two_pi * counts_v[...].astype(f32)
    pl.semaphore_wait(barrier, n * slabs - 1)

    for c in range(chunk_count):
        @pl.loop(0, n - 1)
        def _(step):
            to = partner(me, n - 1 - step // 2 - (step % 2) * (n // 2), n)
            pltpu.make_async_remote_copy(
                src_ref=sent.at[:, pl.ds(pl.multiple_of(to * columns + starts[c], 128), widths[c])],
                dst_ref=got[c].at[me],
                send_sem=send_sem.at[c],
                recv_sem=recv_sem.at[c],
                device_id={"ifg": to},
                device_id_type=MESH,
            ).start()

    own = [
        pltpu.make_async_copy(
            sent.at[:, pl.ds(pl.multiple_of(me * columns + starts[c], 128), widths[c])], got[c].at[me], own_sem.at[c]
        )
        for c in range(chunk_count)
    ]
    for copy in own:
        copy.start()

    eye_bool = lax.broadcasted_iota(jnp.int32, (dates, dates), 0) == lax.broadcasted_iota(
        jnp.int32, (dates, dates), 1
    )
    eye = eye_bool.astype(f32)
    for copy in tables:
        copy.wait()
    loop_count = loops.shape[0]
    left[0:loop_count, :] = loops_v[...].astype(f32).astype(bf16)
    left[loop_count:, :] = design_v[...].astype(f32).astype(bf16)
    design_b[...] = jnp.transpose(design_v[...].astype(f32)).astype(bf16)
    matrix = dot(left[loop_count:, :], design_b[...]) + ridge_weight * eye
    normal[...] = matrix
    bound = jnp.max(jnp.sum(jnp.abs(matrix), axis=1, keepdims=True), axis=0, keepdims=True)
    scale = 2.0 / (bound + ridge_weight)
    stack[0:dates, :] = scale * eye
    stack[dates:, :] = eye - scale * matrix

    @pl.loop(0, doublings)
    def _(step):
        both = stack[...]
        product = dot_split(both, both[dates:, :])
        stack[0:dates, :] = both[0:dates, :] + product[0:dates, :]
        stack[dates:, :] = product[dates:, :]

    @pl.loop(0, newton_steps)
    def _(step):
        inverse = stack[0:dates, :]
        error = eye - jnp.dot(normal[...], inverse, precision=highest)
        stack[0:dates, :] = inverse + jnp.dot(inverse, error, precision=highest)

    squares = jnp.zeros((1, 128), f32)
    date_sums = jnp.zeros((8, dates), f32)
    for c in range(chunk_count):
        width = widths[c]
        own[c].wait()
        pltpu.make_async_copy(got[c].at[pl.ds(0, n - 1)], got[c].at[pl.ds(0, n - 1)], recv_sem.at[c]).wait()
        if rows % 8 == 0:
            held = got[c][...].reshape(n * rows, width)
        else:
            for source in range(n):
                flat[source * rows:(source + 1) * rows, 0:width] = got[c][source]
            held = flat[:, 0:width]
        triple = dot(left[...], jnp.concatenate(split_three(held), axis=1))
        summed = triple[:, 0:width] + (triple[:, width:2 * width] + triple[:, 2 * width:])
        closure_out[:, starts[c]:starts[c] + width] = summed[0:loop_count, :]
        shifts = jnp.dot(stack[0:dates, :], summed[loop_count:, :], precision=highest)
        shifts_out[:, starts[c]:starts[c] + width] = shifts
        modelled = dot(design_b[...], jnp.concatenate(split_three(shifts), axis=1))
        residual = held - (modelled[:, 0:width] + (modelled[:, width:2 * width] + modelled[:, 2 * width:]))
        line = jnp.sum(residual * residual, axis=0, keepdims=True)
        for part in range(width // 128):
            squares = squares + line[:, part * 128:(part + 1) * 128]
        date_sums = date_sums + lax.dot_general(
            jnp.ones((8, width), f32), shifts, (((1,), (1,)), ((), ())), precision=highest,
            preferred_element_type=f32,
        )

    padded = row.shape[2] - 128
    row[0, :, 0:dates] = date_sums[0:1, :]
    row[0, :, padded:] = squares
    mine = slab * n + me
    rows_in[mine, :, :] = row[0]
    for other in range(slabs):
        far_slab = lax.rem(slab + other, slabs)

        @pl.loop(0 if other else 1, n)
        def _(k):
            pltpu.make_async_remote_copy(
                src_ref=row.at[0],
                dst_ref=rows_in.at[mine],
                send_sem=row_send,
                recv_sem=row_recv,
                device_id={"ifg": partner(me, k, n), "slab": far_slab},
                device_id_type=MESH,
            ).start()

    for c in range(chunk_count):
        pltpu.make_async_copy(got[c].at[pl.ds(0, n - 1)], got[c].at[pl.ds(0, n - 1)], send_sem.at[c]).wait()
    everyone = rows_in.at[pl.ds(0, n * slabs - 1)]
    pltpu.make_async_copy(everyone, everyone, row_recv).wait()
    pltpu.make_async_copy(everyone, everyone, row_send).wait()
    date_total = jnp.sum(rows_in[:, :, 0:dates], axis=0)
    frame_mean = jnp.sum(jnp.where(eye_bool, date_total, 0.0), axis=1, keepdims=True) * (1.0 / (slabs * n * columns))
    shifts_out[...] = shifts_out[...] - frame_mean
    slab_squares = jnp.sum(rows_in[pl.ds(slab * n, n), :, padded:], axis=0)
    slab_square = jnp.sum(slab_squares, axis=1, keepdims=True)
    misfit_out[...] = jnp.sqrt(slab_square * (1.0 / (ifgs * n * columns)) + epsilon)


def local(phase, corrections, closure_loops, design):
    n = lax.axis_size("ifg")
    slabs = lax.axis_size("slab")
    rows, pixels = phase.shape[1:]
    ifgs, dates = design.shape
    loop_count = closure_loops.shape[0]
    columns = pixels // n
    widths = (columns - 128, 128) if columns > 128 else (columns,)
    padded = -(-dates // 128) * 128
    doublings = 1
    while 2 ** doublings < 4 * ifgs:
        doublings += 1
    vmem = pl.BlockSpec(memory_space=pltpu.VMEM)
    in_hbm = pl.BlockSpec(memory_space=pltpu.HBM)
    dma = pltpu.SemaphoreType.DMA
    closure, displacement, misfit = pl.pallas_call(
        functools.partial(kernel, n, slabs, widths, doublings),
        out_shape=(
            jax.ShapeDtypeStruct((loop_count, columns), f32),
            jax.ShapeDtypeStruct((dates, columns), f32),
            jax.ShapeDtypeStruct((1, 1), f32),
        ),
        in_specs=[in_hbm] * 4,
        out_specs=(vmem, vmem, vmem),
        scratch_shapes=[
            pltpu.VMEM((rows, pixels), f32),
            pltpu.VMEM((rows, pixels), jnp.int32),
            pltpu.VMEM((rows, pixels), f32),
            *[pltpu.VMEM((n, rows, width), f32) for width in widths],
            pltpu.VMEM((loop_count, ifgs), jnp.int32),
            pltpu.VMEM((dates, ifgs), jnp.int32),
            pltpu.VMEM((ifgs, dates), bf16),
            pltpu.VMEM((loop_count + dates, ifgs), bf16),
            pltpu.VMEM((2 * dates, dates), f32),
            pltpu.VMEM((dates, dates), f32),
            pltpu.VMEM((1, 1, padded + 128), f32),
            pltpu.VMEM((n * slabs, 1, padded + 128), f32),
            pltpu.VMEM((8 if rows % 8 == 0 else ifgs, max(widths)), f32),
            dma((2,)),
            dma((2,)),
            dma((len(widths),)),
            dma((len(widths),)),
            dma((len(widths),)),
            dma,
            dma,
        ],
        compiler_params=pltpu.CompilerParams(
            collective_id=0, has_side_effects=True, vmem_limit_bytes=65_500_000
        ),
    )(phase, corrections, closure_loops, design.T)
    return (closure[None], displacement[None], misfit.reshape(1))


def solution(mesh):
    in_specs = (P("slab", "ifg", None), P("slab", "ifg", None), P(), P())
    out_specs = (P("slab", None, "ifg"), P("slab", None, "ifg"), P("slab"))
    return jax.shard_map(local, mesh=mesh, in_specs=in_specs, out_specs=out_specs, check_vma=False)
```

```python
import functools

import jax
import jax.numpy as jnp
from jax import lax
from jax.experimental import pallas as pl
from jax.experimental.pallas import tpu as pltpu
from jax.sharding import PartitionSpec as P

ridge_weight = 1.0
two_pi = 6.283185307179586
epsilon = 1e-06
highest = lax.Precision.HIGHEST
f32 = jnp.float32
bf16 = jnp.bfloat16
MESH = pl.DeviceIdType.MESH
newton_steps = 2


def dot(a, b):
    return jnp.dot(a, b, preferred_element_type=f32)


def split(a):
    high = a.astype(bf16)
    return high, (a - high.astype(f32)).astype(bf16)


def split_three(a):
    high = a.astype(bf16)
    rest = a - high.astype(f32)
    middle = rest.astype(bf16)
    return high, middle, (rest - middle.astype(f32)).astype(bf16)


def dot_split(a, b):
    a_high, a_low = split(a)
    b_high, b_low = split(b)
    return dot(a_high, b_high) + (dot(a_high, b_low) + dot(a_low, b_high))


def partner(me, k, n):
    if n & (n - 1):
        return lax.rem(me + k, n)
    out, bit = 0, 1
    while bit < n:
        out = out + bit * (((me // bit) % 2 + (k // bit) % 2) % 2)
        bit *= 2
    return out


def kernel(n, slabs, widths, doublings, phase, counts, loops, design_t, closure_out, shifts_out, misfit_out,
           phase_v, counts_v, sent, *rest):
    chunk_count = len(widths)
    got, rest = rest[:chunk_count], rest[chunk_count:]
    (loops_v, design_v, design_b, left, stack, normal, row, rows_in, flat,
     in_sem, table_sem, own_sem, send_sem, recv_sem, row_send, row_recv) = rest
    me = lax.axis_index("ifg")
    slab = lax.axis_index("slab")
    rows = phase.shape[1]
    dates, ifgs = design_t.shape
    columns = sum(widths)
    starts = [sum(widths[:c]) for c in range(chunk_count)]

    loads = [
        pltpu.make_async_copy(phase.at[0], phase_v, in_sem.at[0]),
        pltpu.make_async_copy(counts.at[0], counts_v, in_sem.at[1]),
    ]
    tables = [
        pltpu.make_async_copy(design_t, design_v, table_sem.at[0]),
        pltpu.make_async_copy(loops, loops_v, table_sem.at[1]),
    ]
    for copy in loads:
        copy.start()

    barrier = pltpu.get_barrier_semaphore()
    for other in range(slabs):
        far_slab = lax.rem(slab + other, slabs)

        @pl.loop(0 if other else 1, n)
        def _(k):
            pl.semaphore_signal(
                barrier, inc=1, device_id={"ifg": partner(me, k, n), "slab": far_slab}, device_id_type=MESH
            )

    for copy in tables:
        copy.start()
    for copy in loads:
        copy.wait()
    sent[...] = phase_v[...] + two_pi * counts_v[...].astype(f32)
    pl.semaphore_wait(barrier, n * slabs - 1)

    for c in range(chunk_count):
        @pl.loop(0, n - 1)
        def _(step):
            to = partner(me, n - 1 - step // 2 - (step % 2) * (n // 2), n)
            pltpu.make_async_remote_copy(
                src_ref=sent.at[:, pl.ds(pl.multiple_of(to * columns + starts[c], 128), widths[c])],
                dst_ref=got[c].at[me],
                send_sem=send_sem.at[c],
                recv_sem=recv_sem.at[c],
                device_id={"ifg": to},
                device_id_type=MESH,
            ).start()

    own = [
        pltpu.make_async_copy(
            sent.at[:, pl.ds(pl.multiple_of(me * columns + starts[c], 128), widths[c])], got[c].at[me], own_sem.at[c]
        )
        for c in range(chunk_count)
    ]
    for copy in own:
        copy.start()

    eye_bool = lax.broadcasted_iota(jnp.int32, (dates, dates), 0) == lax.broadcasted_iota(
        jnp.int32, (dates, dates), 1
    )
    eye = eye_bool.astype(f32)
    for copy in tables:
        copy.wait()
    loop_count = loops.shape[0]
    left[0:loop_count, :] = loops_v[...].astype(f32).astype(bf16)
    left[loop_count:, :] = design_v[...].astype(f32).astype(bf16)
    design_b[...] = jnp.transpose(design_v[...].astype(f32)).astype(bf16)
    matrix = dot(left[loop_count:, :], design_b[...]) + ridge_weight * eye
    normal[...] = matrix
    bound = jnp.max(jnp.sum(jnp.abs(matrix), axis=1, keepdims=True), axis=0, keepdims=True)
    scale = 2.0 / (bound + ridge_weight)
    stack[0:dates, :] = scale * eye
    stack[dates:, :] = eye - scale * matrix

    @pl.loop(0, doublings)
    def _(step):
        both = stack[...]
        product = dot_split(both, both[dates:, :])
        stack[0:dates, :] = both[0:dates, :] + product[0:dates, :]
        stack[dates:, :] = product[dates:, :]

    @pl.loop(0, newton_steps)
    def _(step):
        inverse = stack[0:dates, :]
        error = eye - jnp.dot(normal[...], inverse, precision=highest)
        stack[0:dates, :] = inverse + jnp.dot(inverse, error, precision=highest)

    squares = jnp.zeros((1, 128), f32)
    date_sums = jnp.zeros((8, dates), f32)
    for c in range(chunk_count):
        width = widths[c]
        own[c].wait()
        pltpu.make_async_copy(got[c].at[pl.ds(0, n - 1)], got[c].at[pl.ds(0, n - 1)], recv_sem.at[c]).wait()
        if rows % 8 == 0:
            held = got[c][...].reshape(n * rows, width)
        else:
            for source in range(n):
                flat[source * rows:(source + 1) * rows, 0:width] = got[c][source]
            held = flat[:, 0:width]
        triple = dot(left[...], jnp.concatenate(split_three(held), axis=1))
        summed = triple[:, 0:width] + (triple[:, width:2 * width] + triple[:, 2 * width:])
        closure_out[:, starts[c]:starts[c] + width] = summed[0:loop_count, :]
        shifts = jnp.dot(stack[0:dates, :], summed[loop_count:, :], precision=highest)
        shifts_out[:, starts[c]:starts[c] + width] = shifts
        modelled = dot(design_b[...], jnp.concatenate(split_three(shifts), axis=1))
        residual = held - (modelled[:, 0:width] + (modelled[:, width:2 * width] + modelled[:, 2 * width:]))
        line = jnp.sum(residual * residual, axis=0, keepdims=True)
        for part in range(width // 128):
            squares = squares + line[:, part * 128:(part + 1) * 128]
        date_sums = date_sums + lax.dot_general(
            jnp.ones((8, width), f32), shifts, (((1,), (1,)), ((), ())), precision=highest,
            preferred_element_type=f32,
        )

    padded = row.shape[2] - 128
    row[0, :, 0:dates] = date_sums[0:1, :]
    row[0, :, padded:] = squares
    mine = slab * n + me
    rows_in[mine, :, :] = row[0]
    for other in range(slabs):
        far_slab = lax.rem(slab + other, slabs)

        @pl.loop(0 if other else 1, n)
        def _(k):
            pltpu.make_async_remote_copy(
                src_ref=row.at[0],
                dst_ref=rows_in.at[mine],
                send_sem=row_send,
                recv_sem=row_recv,
                device_id={"ifg": partner(me, k, n), "slab": far_slab},
                device_id_type=MESH,
            ).start()

    for c in range(chunk_count):
        pltpu.make_async_copy(got[c].at[pl.ds(0, n - 1)], got[c].at[pl.ds(0, n - 1)], send_sem.at[c]).wait()
    everyone = rows_in.at[pl.ds(0, n * slabs - 1)]
    pltpu.make_async_copy(everyone, everyone, row_recv).wait()
    pltpu.make_async_copy(everyone, everyone, row_send).wait()
    date_total = jnp.sum(rows_in[:, :, 0:dates], axis=0)
    frame_mean = jnp.sum(jnp.where(eye_bool, date_total, 0.0), axis=1, keepdims=True) * (1.0 / (slabs * n * columns))
    shifts_out[...] = shifts_out[...] - frame_mean
    slab_squares = jnp.sum(rows_in[pl.ds(slab * n, n), :, padded:], axis=0)
    slab_square = jnp.sum(slab_squares, axis=1, keepdims=True)
    misfit_out[...] = jnp.sqrt(slab_square * (1.0 / (ifgs * n * columns)) + epsilon)


def local(phase, corrections, closure_loops, design):
    n = lax.axis_size("ifg")
    slabs = lax.axis_size("slab")
    rows, pixels = phase.shape[1:]
    ifgs, dates = design.shape
    loop_count = closure_loops.shape[0]
    columns = pixels // n
    widths = (columns - 128, 128) if columns > 128 else (columns,)
    padded = -(-dates // 128) * 128
    doublings = 1
    while 2 ** doublings < 4 * ifgs:
        doublings += 1
    vmem = pl.BlockSpec(memory_space=pltpu.VMEM)
    in_hbm = pl.BlockSpec(memory_space=pltpu.HBM)
    dma = pltpu.SemaphoreType.DMA
    closure, displacement, misfit = pl.pallas_call(
        functools.partial(kernel, n, slabs, widths, doublings),
        out_shape=(
            pltpu.VMEM((loop_count, columns), f32),
            pltpu.VMEM((dates, columns), f32),
            jax.ShapeDtypeStruct((1, 1), f32),
        ),
        in_specs=[in_hbm] * 4,
        out_specs=(vmem, vmem, vmem),
        scratch_shapes=[
            pltpu.VMEM((rows, pixels), f32),
            pltpu.VMEM((rows, pixels), jnp.int32),
            pltpu.VMEM((rows, pixels), f32),
            *[pltpu.VMEM((n, rows, width), f32) for width in widths],
            pltpu.VMEM((loop_count, ifgs), jnp.int32),
            pltpu.VMEM((dates, ifgs), jnp.int32),
            pltpu.VMEM((ifgs, dates), bf16),
            pltpu.VMEM((loop_count + dates, ifgs), bf16),
            pltpu.VMEM((2 * dates, dates), f32),
            pltpu.VMEM((dates, dates), f32),
            pltpu.VMEM((1, 1, padded + 128), f32),
            pltpu.VMEM((n * slabs, 1, padded + 128), f32),
            pltpu.VMEM((8 if rows % 8 == 0 else ifgs, max(widths)), f32),
            dma((2,)),
            dma((2,)),
            dma((len(widths),)),
            dma((len(widths),)),
            dma((len(widths),)),
            dma,
            dma,
        ],
        compiler_params=pltpu.CompilerParams(
            collective_id=0, has_side_effects=True, vmem_limit_bytes=62_000_000
        ),
    )(phase, corrections, closure_loops, design.T)
    return (closure[None], displacement[None], misfit.reshape(1))


def solution(mesh):
    in_specs = (P("slab", "ifg", None), P("slab", "ifg", None), P(), P())
    out_specs = (P("slab", None, "ifg"), P("slab", None, "ifg"), P("slab"))
    return jax.shard_map(local, mesh=mesh, in_specs=in_specs, out_specs=out_specs, check_vma=False)
```
